16 devices in a mesh: rep: 2 (over y, z), pp: 8 (over x, core).
Axes of the slice: x: 4, y: 2, z: 1, core: 2. Of those that a mesh axis runs over, the one named last changes fastest.
The devices are a block of a 4x4x8 slice.
Arguments:
- x: bfloat16 [32, 512, 512], P('rep'), parts along dimension 0
- dy: bfloat16 [32, 512, 512], P('rep'), parts along dimension 0
- w_gate: bfloat16 [8, 512, 1408], P('pp')
- w_up: bfloat16 [8, 512, 1408], P('pp')
- w_down: bfloat16 [8, 1408, 512], P('pp')
Outputs:
- output 1: bfloat16 [16, 512, 1408], P(('rep', 'pp')), parts along dimension 0
- output 2: bfloat16 [16, 512, 1408], P(('rep', 'pp')), parts along dimension 0
- output 3: bfloat16 [16, 1408, 512], P(('rep', 'pp')), parts along dimension 0
There are 2 independent parts. The reference program is written for one: setup_inputs(seed, part) draws one part's arguments, and reference() takes and returns one part's arrays. A program takes and returns all parts, laid end to end along the dimension named above; an argument that names none is the same for every part.
All inputs are finite; a program needn't handle non-finite values.
Results may differ from the reference program's by a relative error of at most 0.0298.
Values are sent between devices in bfloat16 or wider.
A program may use at most 768 MiB of HBM per device.

```python
import jax
import jax.numpy as jnp
from jax import lax

MICRO = 16
TOKENS = 512
D = 512
FF = 1408
LAYERS = 8
NAMES = ("w_gate", "w_up", "w_down")
SHAPES = {"w_gate": (LAYERS, D, FF), "w_up": (LAYERS, D, FF), "w_down": (LAYERS, FF, D)}


def bump(key, n, height):
    away = (jnp.arange(n, dtype=jnp.int32) - jax.random.randint(key, (), 0, n, jnp.int32)) % n
    return jnp.where(away < n // 8, height, 1.0)


def together(key, own, strength):
    shared = jax.random.normal(key, own.shape[1:], jnp.float32)
    return (own + strength * shared) * lax.rsqrt(1 + strength * strength)


def setup_inputs(seed: int = 0, part: int = 0) -> dict:
    kx, kdy, ka, kb, kz, kf, kh, kl, *kw = jax.random.split(jax.random.key(seed), 8 + len(NAMES))
    kx, kdy, ka, kb = (jax.random.fold_in(k, part) for k in (kx, kdy, ka, kb))
    shape = (MICRO, TOKENS, D)
    much_x, much_dy = jax.random.uniform(kz, (2,), jnp.float32, 0.0, 1.0)
    layers = 2.0 ** jax.random.uniform(kl, (LAYERS, 1, 1), jnp.float32, -1.0, 1.0)
    x = together(ka, jax.random.normal(kx, shape, jnp.float32), much_x) * bump(kf, D, 4.0)
    dy = together(kb, jax.random.normal(kdy, shape, jnp.float32), much_dy)
    drawn = {"x": x.astype(jnp.bfloat16), "dy": (dy * (MICRO * TOKENS) ** -0.5).astype(jnp.bfloat16)}
    for key, name in zip(kw, NAMES, strict=True):
        w = jax.random.normal(key, SHAPES[name], jnp.float32) * SHAPES[name][1] ** -0.5
        drawn[name] = (w * {"w_gate": 1.0, "w_up": bump(kh, FF, 4.0), "w_down": layers}[name]).astype(jnp.bfloat16)
    return drawn


def matmul(a, w):
    return jnp.dot(a, w, preferred_element_type=jnp.float32).astype(jnp.bfloat16)


def normed(h):
    wide = h.astype(jnp.float32)
    scale = lax.rsqrt(jnp.mean(wide**2, -1, keepdims=True) + 1e-6)
    return (wide * scale).astype(jnp.bfloat16)


def layer(h, w):
    a = normed(h)
    gate = jnp.dot(a, w["w_gate"], preferred_element_type=jnp.float32)
    up = jnp.dot(a, w["w_up"], preferred_element_type=jnp.float32)
    return h + matmul((jax.nn.silu(gate) * up).astype(jnp.bfloat16), w["w_down"])


def stack(weights, h):
    return lax.scan(lambda h, w: (layer(h, w), None), h, weights)[0]


def reference(x, dy, w_gate, w_up, w_down):
    weights = dict(zip(NAMES, (w_gate, w_up, w_down), strict=True))

    def take(so_far, one):
        h, by_y = one
        _, back = jax.vjp(lambda w: stack(w, h), weights)
        return jax.tree.map(lambda total, term: total + term.astype(jnp.float32), so_far, back(by_y)[0]), None

    none_yet = {name: jnp.zeros(w.shape, jnp.float32) for name, w in weights.items()}
    by_weights, _ = lax.scan(take, none_yet, (x, dy))
    return tuple(by_weights[name].astype(jnp.bfloat16) for name in NAMES)
```

```python
import functools

import jax
import jax.numpy as jnp
from jax import lax
from jax.experimental import pallas as pl
from jax.experimental.pallas import tpu as pltpu
from jax.sharding import PartitionSpec as P

MESH = pl.DeviceIdType.MESH
F32, BF16 = jnp.float32, jnp.bfloat16
BLOCKS = 2
LANES = 128
AHEAD = 2
LAG = 2
SENDS = 4
EPS = 1e-6


def dot(a, b):
    return jnp.dot(a, b, preferred_element_type=F32)


def kernel(
    stages, micro, blocks,
    x_ref, dy_ref, wg_ref, wu_ref, wd_ref, dgu_out, dwd_out,
    wgu, wd, wgu_t, wd_t, hs, norms, grads, fsend, bsend, act_tmp, acts, dgus, turned, acc_gu, acc_d,
    w_sem, wd_sem, out_sem, recv_f, recv_b, send_f, send_b,
):
    me = lax.axis_index("pp")
    rows, d = hs.shape[1:]
    ff = wd.shape[0]
    first, last = me == 0, me == stages - 1
    pieces = ff // LANES
    wide = [(c, min(2 * LANES, ff - c)) for c in range(0, ff, 2 * LANES)]

    for c in range(pieces):
        at = pl.ds(c * LANES, LANES)
        pltpu.make_async_copy(wg_ref.at[0, :, at], wgu.at[:, pl.ds(2 * c * LANES, LANES)], w_sem).start()
        pltpu.make_async_copy(wu_ref.at[0, :, at], wgu.at[:, pl.ds((2 * c + 1) * LANES, LANES)], w_sem).start()
    pltpu.make_async_copy(wd_ref.at[0], wd, wd_sem).start()

    def x_copy(b):
        return pltpu.make_async_copy(x_ref.at[b], hs.at[b], recv_f.at[b])

    def dy_copy(b):
        return pltpu.make_async_copy(dy_ref.at[b], grads.at[b], recv_b.at[b])

    def f_copy(b):
        slot = lax.rem(b, SENDS)
        return pltpu.make_async_remote_copy(
            src_ref=fsend.at[slot], dst_ref=hs.at[b], send_sem=send_f.at[slot], recv_sem=recv_f.at[b],
            device_id={"pp": me + 1}, device_id_type=MESH,
        )

    def b_copy(b):
        slot = lax.rem(b, SENDS)
        return pltpu.make_async_remote_copy(
            src_ref=bsend.at[slot], dst_ref=grads.at[b], send_sem=send_b.at[slot], recv_sem=recv_b.at[b],
            device_id={"pp": me - 1}, device_id_type=MESH,
        )

    barrier = pltpu.get_barrier_semaphore()

    @pl.when(me > 0)
    def _():
        pl.semaphore_signal(barrier, inc=1, device_id={"pp": me - 1}, device_id_type=MESH)

    @pl.when(me < stages - 1)
    def _():
        pl.semaphore_signal(barrier, inc=1, device_id={"pp": me + 1}, device_id_type=MESH)

    total_blocks = micro * blocks

    @pl.when(first)
    def _():
        @pl.loop(0, total_blocks)
        def _(b):
            x_copy(b).start()

    @pl.when(last)
    def _():
        @pl.loop(0, total_blocks)
        def _(b):
            dy_copy(b).start()

    acc_gu[...] = jnp.zeros_like(acc_gu)
    acc_d[...] = jnp.zeros_like(acc_d)
    pltpu.make_async_copy(wgu, wgu, w_sem).wait()
    pltpu.make_async_copy(wd_ref.at[0], wd, wd_sem).wait()

    def turn_weights():
        for c in range(pieces):
            at = pl.ds(c * LANES, LANES)
            wd_t[:, at] = wd[at, :].T
        for c in range(2 * pieces):
            at = pl.ds(c * LANES, LANES)
            wgu_t[at, :] = wgu[:, at].T

    @pl.when(me > 0)
    def _():
        turn_weights()

    pl.semaphore_wait(barrier, jnp.where(first | last, 1, 2))

    def gated(gu, n):
        g = jnp.concatenate([gu[:, 2 * i * LANES:(2 * i + 1) * LANES] for i in range(n)], axis=1)
        u = jnp.concatenate([gu[:, (2 * i + 1) * LANES:(2 * i + 2) * LANES] for i in range(n)], axis=1)
        return g, u, 0.5 * jnp.tanh(0.5 * g) + 0.5

    def forward(b):
        @pl.when(first)
        def _():
            x_copy(b).wait()

        @pl.when(me > 0)
        def _():
            f_copy(b).wait_recv()

        h = hs[b].astype(F32)
        scale = lax.rsqrt(jnp.mean(h * h, -1, keepdims=True) + EPS)
        a = (h * scale).astype(BF16)
        norms[b] = a

        @pl.when(me < stages - 1)
        def _():
            @pl.when(b >= SENDS)
            def _():
                f_copy(b - SENDS).wait_send()

            for c, w in wide:
                gu = dot(norms[b], wgu[:, 2 * c:2 * c + 2 * w])
                g, u, s = gated(gu, w // LANES)
                act_tmp[:, c:c + w] = (g * s * u).astype(BF16)
            y = dot(act_tmp[...], wd[...]).astype(BF16)
            fsend[lax.rem(b, SENDS)] = (hs[b].astype(F32) + y.astype(F32)).astype(BF16)
            f_copy(b).start()

    def backward(b, ring):
        @pl.when(last)
        def _():
            dy_copy(b).wait()

        @pl.when(me < stages - 1)
        def _():
            pltpu.make_async_remote_copy(
                src_ref=bsend.at[0], dst_ref=grads.at[b], send_sem=send_b.at[0], recv_sem=recv_b.at[b],
                device_id={"pp": me + 1}, device_id_type=MESH,
            ).wait_recv()

        part = lax.rem(b, blocks)
        slot = ring * blocks + part
        for c, w in wide:
            gu = dot(norms[b], wgu[:, 2 * c:2 * c + 2 * w])
            dact = dot(grads[b], wd_t[:, c:c + w]).astype(BF16).astype(F32)
            g, u, s = gated(gu, w // LANES)
            silu = g * s
            acts[slot, :, c:c + w] = (silu * u).astype(BF16)
            dup = dact * silu
            dgate = dact * u * (s + silu * (1.0 - s))
            both = []
            for i in range(w // LANES):
                both += [dgate[:, i * LANES:(i + 1) * LANES], dup[:, i * LANES:(i + 1) * LANES]]
            dgus[slot, :, 2 * c:2 * c + 2 * w] = jnp.concatenate(both, axis=1).astype(BF16)

        @pl.when(me > 0)
        def _():
            @pl.when(b >= SENDS)
            def _():
                b_copy(b - SENDS).wait_send()

            da = dot(dgus[slot], wgu_t[...]).astype(BF16).astype(F32)
            h = hs[b].astype(F32)
            scale = lax.rsqrt(jnp.mean(h * h, -1, keepdims=True) + EPS)
            pull = jnp.mean(da * h, -1, keepdims=True) * (scale * scale * scale)
            dh = (da * scale - h * pull).astype(BF16).astype(F32)
            bsend[lax.rem(b, SENDS)] = (grads[b].astype(F32) + dh).astype(BF16)
            b_copy(b).start()

    tokens = rows * blocks

    def whole(ref, start, cols):
        return ref[pl.ds(start, blocks), :, cols].reshape(tokens, -1)

    def weight(k, ring):
        turned[0] = whole(norms, k * blocks, slice(None)).T
        turned[1] = whole(grads, k * blocks, slice(None)).T
        base = ring * blocks
        for c in range(0, 2 * ff, 2 * LANES):
            term = dot(turned[0], whole(dgus, base, slice(c, c + 2 * LANES)))
            acc_gu[:, c:c + 2 * LANES] += term.astype(BF16).astype(F32)
        for c, w in wide:
            term = dot(turned[1], whole(acts, base, slice(c, c + w)))
            acc_d[:, c:c + w] += term.astype(BF16).astype(F32)

    ahead = AHEAD * (stages - 1 - me)
    ahead = jnp.minimum(ahead, micro)

    @pl.loop(0, micro + min(AHEAD * (stages - 1), micro) + LAG)
    def _(t):
        @pl.when(first & (t == micro // 2))
        def _():
            turn_weights()

        @pl.when(t < micro)
        def _():
            @pl.loop(0, blocks)
            def _(j):
                forward(t * blocks + j)

        kb = t - ahead

        @pl.when((kb >= 0) & (kb < micro))
        def _():
            @pl.loop(0, blocks)
            def _(j):
                backward(kb * blocks + j, lax.rem(kb, LAG + 1))

        kw = kb - LAG

        @pl.when((kw >= 0) & (kw < micro))
        def _():
            weight(kw, lax.rem(kw, LAG + 1))

    copies = []
    for j in range(blocks):
        at = pl.ds(j * rows, rows)
        dgus[j] = acc_gu[j * rows:(j + 1) * rows, :].astype(BF16)
        acts[j] = acc_d[j * rows:(j + 1) * rows, :].astype(BF16)
        copies.append(pltpu.make_async_copy(dgus.at[j], dgu_out.at[at], out_sem.at[2 * j]))
        copies.append(pltpu.make_async_copy(acts.at[j], dwd_out.at[at], out_sem.at[2 * j + 1]))
        copies[-2].start()
        copies[-1].start()

    @pl.when(me < stages - 1)
    def _():
        @pl.loop(total_blocks - SENDS, total_blocks)
        def _(b):
            f_copy(b).wait_send()

    @pl.when(me > 0)
    def _():
        @pl.loop(total_blocks - SENDS, total_blocks)
        def _(b):
            b_copy(b).wait_send()

    for copy in copies:
        copy.wait()


def solution(mesh):
    stages = mesh.shape["pp"]

    def step(x, dy, w_gate, w_up, w_down):
        micro, tokens, d = x.shape
        ff = w_gate.shape[-1]
        rows = tokens // BLOCKS
        count = micro * BLOCKS
        ring = (LAG + 1) * BLOCKS
        any_space = pl.BlockSpec(memory_space=pl.ANY)
        dgu, dwd = pl.pallas_call(
            functools.partial(kernel, stages, micro, BLOCKS),
            out_shape=(jax.ShapeDtypeStruct((d, 2 * ff), BF16), jax.ShapeDtypeStruct((d, ff), BF16)),
            in_specs=[any_space] * 5,
            out_specs=(any_space,) * 2,
            scratch_shapes=[
                pltpu.VMEM((d, 2 * ff), BF16),
                pltpu.VMEM((ff, d), BF16),
                pltpu.VMEM((2 * ff, d), BF16),
                pltpu.VMEM((d, ff), BF16),
                pltpu.VMEM((count, rows, d), BF16),
                pltpu.VMEM((count, rows, d), BF16),
                pltpu.VMEM((count, rows, d), BF16),
                pltpu.VMEM((SENDS, rows, d), BF16),
                pltpu.VMEM((SENDS, rows, d), BF16),
                pltpu.VMEM((rows, ff), BF16),
                pltpu.VMEM((ring, rows, ff), BF16),
                pltpu.VMEM((ring, rows, 2 * ff), BF16),
                pltpu.VMEM((2, d, tokens), BF16),
                pltpu.VMEM((d, 2 * ff), F32),
                pltpu.VMEM((d, ff), F32),
                pltpu.SemaphoreType.DMA,
                pltpu.SemaphoreType.DMA,
                pltpu.SemaphoreType.DMA((2 * BLOCKS,)),
                pltpu.SemaphoreType.DMA((count,)),
                pltpu.SemaphoreType.DMA((count,)),
                pltpu.SemaphoreType.DMA((SENDS,)),
                pltpu.SemaphoreType.DMA((SENDS,)),
            ],
            compiler_params=pltpu.CompilerParams(collective_id=0, has_side_effects=True, vmem_limit_bytes=67_043_328),
            name="stage",
        )(x.reshape(count, rows, d), dy.reshape(count, rows, d), w_gate, w_up, w_down)
        pairs = dgu.reshape(d, ff // LANES, 2, LANES)
        return pairs[:, :, 0].reshape(1, d, ff), pairs[:, :, 1].reshape(1, d, ff), dwd.T[None]

    return jax.shard_map(
        step,
        mesh=mesh,
        in_specs=(P("rep", None, None),) * 2 + (P("pp", None, None),) * 3,
        out_specs=(P(("rep", "pp"), None, None),) * 3,
        check_vma=False,
    )
```

```python
import functools

import jax
import jax.numpy as jnp
from jax import lax
from jax.experimental import pallas as pl
from jax.experimental.pallas import tpu as pltpu
from jax.sharding import PartitionSpec as P

MESH = pl.DeviceIdType.MESH
F32, BF16 = jnp.float32, jnp.bfloat16
BLOCKS = 2
LANES = 128
AHEAD = 2
LAG = 0
SENDS = 4
EPS = 1e-6


def dot(a, b):
    return jnp.dot(a, b, preferred_element_type=F32)


def kernel(
    stages, micro, blocks,
    x_ref, dy_ref, wg_ref, wu_ref, wd_ref, out_g, out_u, out_d, slopes_hbm, acts_hbm,
    wgu, wd, wgu_t, wd_t, hs, norms, grads, fsend, bsend, slopes, acts, dgus, turned, acc_gu, acc_d,
    w_sem, wd_sem, out_sem, recv_f, recv_b, send_f, send_b, put_s, put_a, get_s, get_a,
):
    me = lax.axis_index("pp")
    rows, d = hs.shape[1:]
    ff = wd.shape[0]
    first, last = me == 0, me == stages - 1
    pieces = ff // LANES
    wide = [(c, min(2 * LANES, ff - c)) for c in range(0, ff, 2 * LANES)]
    total_blocks = micro * blocks
    ring = (LAG + 1) * blocks

    def x_copy(b):
        return pltpu.make_async_copy(x_ref.at[b], hs.at[b], recv_f.at[b])

    def dy_copy(b):
        return pltpu.make_async_copy(dy_ref.at[b], grads.at[b], recv_b.at[b])

    def f_copy(b):
        slot = lax.rem(b, SENDS)
        return pltpu.make_async_remote_copy(
            src_ref=fsend.at[slot], dst_ref=hs.at[b], send_sem=send_f.at[slot], recv_sem=recv_f.at[b],
            device_id={"pp": me + 1}, device_id_type=MESH,
        )

    def b_copy(b):
        slot = lax.rem(b, SENDS)
        return pltpu.make_async_remote_copy(
            src_ref=bsend.at[slot], dst_ref=grads.at[b], send_sem=send_b.at[slot], recv_sem=recv_b.at[b],
            device_id={"pp": me - 1}, device_id_type=MESH,
        )

    def put_slopes(b):
        slot = lax.rem(b, 2)
        return pltpu.make_async_copy(slopes.at[2 + slot], slopes_hbm.at[b], put_s.at[slot])

    def put_acts(b):
        slot = lax.rem(b, 2)
        return pltpu.make_async_copy(acts.at[ring + slot], acts_hbm.at[b], put_a.at[slot])

    def get_slopes(b):
        slot = lax.rem(b, 2)
        return pltpu.make_async_copy(slopes_hbm.at[b], slopes.at[slot], get_s.at[slot])

    def get_acts(b):
        slot = lax.rem(b, ring)
        return pltpu.make_async_copy(acts_hbm.at[b], acts.at[slot], get_a.at[slot])

    @pl.when(first)
    def _():
        x_copy(0).start()

    for c in range(pieces):
        at = pl.ds(c * LANES, LANES)
        pltpu.make_async_copy(wg_ref.at[0, :, at], wgu.at[:, pl.ds(2 * c * LANES, LANES)], w_sem).start()
        pltpu.make_async_copy(wu_ref.at[0, :, at], wgu.at[:, pl.ds((2 * c + 1) * LANES, LANES)], w_sem).start()
    pltpu.make_async_copy(wd_ref.at[0], wd, wd_sem).start()

    barrier = pltpu.get_barrier_semaphore()

    @pl.when(me > 0)
    def _():
        pl.semaphore_signal(barrier, inc=1, device_id={"pp": me - 1}, device_id_type=MESH)

    @pl.when(me < stages - 1)
    def _():
        pl.semaphore_signal(barrier, inc=1, device_id={"pp": me + 1}, device_id_type=MESH)

    @pl.when(first)
    def _():
        @pl.loop(1, total_blocks)
        def _(b):
            x_copy(b).start()

    @pl.when(last)
    def _():
        @pl.loop(0, total_blocks)
        def _(b):
            dy_copy(b).start()

    pltpu.make_async_copy(wgu, wgu, w_sem).wait()
    pltpu.make_async_copy(wd_ref.at[0], wd, wd_sem).wait()

    def turn_weights():
        acc_gu[...] = jnp.zeros_like(acc_gu)
        acc_d[...] = jnp.zeros_like(acc_d)
        for c in range(pieces):
            at = pl.ds(c * LANES, LANES)
            wd_t[:, at] = wd[at, :].T
        for c in range(2 * pieces):
            at = pl.ds(c * LANES, LANES)
            wgu_t[at, :] = wgu[:, at].T

    @pl.when(me > 0)
    def _():
        turn_weights()

    pl.semaphore_wait(barrier, jnp.where(first | last, 1, 2))

    def gated(gu, n):
        g = jnp.concatenate([gu[:, 2 * i * LANES:(2 * i + 1) * LANES] for i in range(n)], axis=1)
        u = jnp.concatenate([gu[:, (2 * i + 1) * LANES:(2 * i + 2) * LANES] for i in range(n)], axis=1)
        return g, u, 0.5 * jnp.tanh(0.5 * g) + 0.5

    def forward(b):
        @pl.when(first)
        def _():
            x_copy(b).wait()

        @pl.when(me > 0)
        def _():
            f_copy(b).wait_recv()

        h = hs[b].astype(F32)
        scale = lax.rsqrt(jnp.mean(h * h, -1, keepdims=True) + EPS)
        a = (h * scale).astype(BF16)
        norms[b] = a

        @pl.when((me < stages - 1) & (b >= 2))
        def _():
            put_slopes(b - 2).wait()
            put_acts(b - 2).wait()

        to_s = jnp.where(last, lax.rem(b, 2), 2 + lax.rem(b, 2))
        to_a = jnp.where(last, lax.rem(b, ring), ring + lax.rem(b, 2))
        for c, w in wide:
            gu = dot(norms[b], wgu[:, 2 * c:2 * c + 2 * w])
            g, u, s = gated(gu, w // LANES)
            silu = g * s
            slopes[to_s, :, c:c + w] = silu
            slopes[to_s, :, ff + c:ff + c + w] = u * (s + silu * (1.0 - s))
            acts[to_a, :, c:c + w] = (silu * u).astype(BF16)

        @pl.when(me < stages - 1)
        def _():
            put_slopes(b).start()
            put_acts(b).start()

            @pl.when(b >= SENDS)
            def _():
                f_copy(b - SENDS).wait_send()

            y = dot(acts[to_a], wd[...]).astype(BF16)
            fsend[lax.rem(b, SENDS)] = (hs[b].astype(F32) + y.astype(F32)).astype(BF16)
            f_copy(b).start()

    def backward(b):
        @pl.when(last)
        def _():
            dy_copy(b).wait()

        @pl.when(me < stages - 1)
        def _():
            get_acts(b).start()

            @pl.when(b + 1 < total_blocks)
            def _():
                get_slopes(b + 1).start()

            pltpu.make_async_remote_copy(
                src_ref=bsend.at[0], dst_ref=grads.at[b], send_sem=send_b.at[0], recv_sem=recv_b.at[b],
                device_id={"pp": me + 1}, device_id_type=MESH,
            ).wait_recv()
            get_slopes(b).wait()

        at_s, slot = lax.rem(b, 2), lax.rem(b, ring)
        for c, w in wide:
            dact = dot(grads[b], wd_t[:, c:c + w]).astype(BF16).astype(F32)
            dgate = (dact * slopes[at_s, :, ff + c:ff + c + w]).astype(BF16)
            dup = (dact * slopes[at_s, :, c:c + w]).astype(BF16)
            for i in range(w // LANES):
                at = 2 * c + 2 * i * LANES
                dgus[slot, :, at:at + LANES] = dgate[:, i * LANES:(i + 1) * LANES]
                dgus[slot, :, at + LANES:at + 2 * LANES] = dup[:, i * LANES:(i + 1) * LANES]

        @pl.when(me > 0)
        def _():
            @pl.when(b >= SENDS)
            def _():
                b_copy(b - SENDS).wait_send()

            da = dot(dgus[slot], wgu_t[...]).astype(BF16).astype(F32)
            h = hs[b].astype(F32)
            scale = lax.rsqrt(jnp.mean(h * h, -1, keepdims=True) + EPS)
            pull = jnp.mean(da * h, -1, keepdims=True) * (scale * scale * scale)
            dh = (da * scale - h * pull).astype(BF16).astype(F32)
            bsend[lax.rem(b, SENDS)] = (grads[b].astype(F32) + dh).astype(BF16)
            b_copy(b).start()

    tokens = rows * blocks

    def whole(ref, start, cols):
        return ref[pl.ds(start, blocks), :, cols].reshape(tokens, -1)

    def weight(k):
        base = lax.rem(k, LAG + 1) * blocks

        @pl.when(me < stages - 1)
        def _():
            @pl.loop(0, blocks)
            def _(j):
                get_acts(k * blocks + j).wait()

        turned[0] = whole(norms, k * blocks, slice(None)).T
        turned[1] = whole(grads, k * blocks, slice(None)).T
        for c in range(0, 2 * ff, 2 * LANES):
            term = dot(turned[0], whole(dgus, base, slice(c, c + 2 * LANES)))
            acc_gu[:, c:c + 2 * LANES] += term.astype(BF16).astype(F32)
        for c, w in wide:
            term = dot(turned[1], whole(acts, base, slice(c, c + w)))
            acc_d[:, c:c + w] += term.astype(BF16).astype(F32)

    ahead = jnp.minimum(AHEAD * (stages - 1 - me), micro)

    @pl.loop(0, micro + min(AHEAD * (stages - 1), micro) + LAG)
    def _(t):
        kb = t - ahead
        kw = kb - LAG

        @pl.when(first & (t == 1))
        def _():
            turn_weights()

        @pl.when((me < stages - 1) & (kb == 0))
        def _():
            get_slopes(0).start()

        @pl.when((me < stages - 1) & (t == micro))
        def _():
            for b in (total_blocks - 2, total_blocks - 1):
                put_slopes(b).wait()
                put_acts(b).wait()

        @pl.loop(0, blocks)
        def _(j):
            @pl.when(t < micro)
            def _():
                forward(t * blocks + j)

            @pl.when((kb >= 0) & (kb < micro))
            def _():
                backward(kb * blocks + j)

        @pl.when((kw >= 0) & (kw < micro))
        def _():
            weight(kw)

    copies = []

    def out(src, dst):
        copies.append(pltpu.make_async_copy(src, dst, out_sem.at[len(copies)]))
        copies[-1].start()

    for j in range(blocks):
        at = slice(j * rows, (j + 1) * rows)
        for c in range(pieces):
            dgus[j, :, c * LANES:(c + 1) * LANES] = acc_gu[at, 2 * c * LANES:(2 * c + 1) * LANES].astype(BF16)
            dgus[j, :, ff + c * LANES:ff + (c + 1) * LANES] = acc_gu[at, (2 * c + 1) * LANES:(2 * c + 2) * LANES].astype(BF16)
        out(dgus.at[j, :, pl.ds(0, ff)], out_g.at[0, pl.ds(j * rows, rows)])
        out(dgus.at[j, :, pl.ds(ff, ff)], out_u.at[0, pl.ds(j * rows, rows)])
    for c in range(pieces):
        at = slice(c * LANES, (c + 1) * LANES)
        wd[at, :] = acc_d[:, at].astype(BF16).T
    out(wd, out_d.at[0])

    @pl.when(me < stages - 1)
    def _():
        @pl.loop(total_blocks - SENDS, total_blocks)
        def _(b):
            f_copy(b).wait_send()

    @pl.when(me > 0)
    def _():
        @pl.loop(total_blocks - SENDS, total_blocks)
        def _(b):
            b_copy(b).wait_send()

    for copy in copies:
        copy.wait()


def solution(mesh):
    stages = mesh.shape["pp"]

    def step(x, dy, w_gate, w_up, w_down):
        micro, tokens, d = x.shape
        ff = w_gate.shape[-1]
        rows = tokens // BLOCKS
        count = micro * BLOCKS
        ring = (LAG + 1) * BLOCKS
        any_space = pl.BlockSpec(memory_space=pl.ANY)
        out_g, out_u, out_d, _, _ = pl.pallas_call(
            functools.partial(kernel, stages, micro, BLOCKS),
            out_shape=(
                jax.ShapeDtypeStruct((1, d, ff), BF16),
                jax.ShapeDtypeStruct((1, d, ff), BF16),
                jax.ShapeDtypeStruct((1, ff, d), BF16),
                jax.ShapeDtypeStruct((count, rows, 2 * ff), F32),
                jax.ShapeDtypeStruct((count, rows, ff), BF16),
            ),
            in_specs=[any_space] * 5,
            out_specs=(any_space,) * 5,
            scratch_shapes=[
                pltpu.VMEM((d, 2 * ff), BF16),
                pltpu.VMEM((ff, d), BF16),
                pltpu.VMEM((2 * ff, d), BF16),
                pltpu.VMEM((d, ff), BF16),
                pltpu.VMEM((count, rows, d), BF16),
                pltpu.VMEM((count, rows, d), BF16),
                pltpu.VMEM((count, rows, d), BF16),
                pltpu.VMEM((SENDS, rows, d), BF16),
                pltpu.VMEM((SENDS, rows, d), BF16),
                pltpu.VMEM((4, rows, 2 * ff), F32),
                pltpu.VMEM((ring + 2, rows, ff), BF16),
                pltpu.VMEM((ring, rows, 2 * ff), BF16),
                pltpu.VMEM((2, d, tokens), BF16),
                pltpu.VMEM((d, 2 * ff), F32),
                pltpu.VMEM((d, ff), F32),
                pltpu.SemaphoreType.DMA,
                pltpu.SemaphoreType.DMA,
                pltpu.SemaphoreType.DMA((2 * BLOCKS + 1,)),
                pltpu.SemaphoreType.DMA((count,)),
                pltpu.SemaphoreType.DMA((count,)),
                pltpu.SemaphoreType.DMA((SENDS,)),
                pltpu.SemaphoreType.DMA((SENDS,)),
                pltpu.SemaphoreType.DMA((2,)),
                pltpu.SemaphoreType.DMA((2,)),
                pltpu.SemaphoreType.DMA((2,)),
                pltpu.SemaphoreType.DMA((ring,)),
            ],
            compiler_params=pltpu.CompilerParams(collective_id=0, has_side_effects=True, vmem_limit_bytes=67_043_328),
            name="stage",
        )(x.reshape(count, rows, d), dy.reshape(count, rows, d), w_gate, w_up, w_down)
        return out_g, out_u, out_d

    return jax.shard_map(
        step,
        mesh=mesh,
        in_specs=(P("rep", None, None),) * 2 + (P("pp", None, None),) * 3,
        out_specs=(P(("rep", "pp"), None, None),) * 3,
        check_vma=False,
    )
```

```python
import functools

import jax
import jax.numpy as jnp
from jax import lax
from jax.experimental import pallas as pl
from jax.experimental.pallas import tpu as pltpu
from jax.sharding import PartitionSpec as P

MESH = pl.DeviceIdType.MESH
F32, BF16 = jnp.float32, jnp.bfloat16
BLOCKS = 2
LANES = 128
AHEAD = (30, 26, 19, 16, 11, 9, 5, 1)
LAG = (4, 4, 12, 14, 19, 21, 32, 31)
SENDS = 4
IN, OUT = 3, 2
EPS = 1e-6


def dot(a, b):
    return jnp.dot(a, b, preferred_element_type=F32)


def kernel(
    stages, micro, blocks,
    x_ref, dy_ref, wg_ref, wu_ref, wd_ref, out_g, out_u, out_d, slopes_hbm, acts_hbm, dgus_hbm,
    wgu, wd, wgu_t, wd_t, hs, grads, fsend, bsend, slopes, acts, dgus, acts_in, dgus_in, turned, acc_gu, acc_d,
    w_sem, wd_sem, out_sem, recv_f, recv_b, send_f, send_b, put_s, put_a, put_d, get_s, get_a, get_d,
):
    me = lax.axis_index("pp")
    rows, d = hs.shape[1:]
    ff = wd.shape[0]
    first, last = me == 0, me == stages - 1
    pieces = ff // LANES
    wide = [(c, min(2 * LANES, ff - c)) for c in range(0, ff, 2 * LANES)]
    total_blocks = micro * blocks

    def x_copy(b):
        return pltpu.make_async_copy(x_ref.at[b], hs.at[b], recv_f.at[b])

    def dy_copy(b):
        return pltpu.make_async_copy(dy_ref.at[b], grads.at[b], recv_b.at[b])

    def f_copy(b):
        slot = lax.rem(b, SENDS)
        return pltpu.make_async_remote_copy(
            src_ref=fsend.at[slot], dst_ref=hs.at[b], send_sem=send_f.at[slot], recv_sem=recv_f.at[b],
            device_id={"pp": me + 1}, device_id_type=MESH,
        )

    def b_copy(b):
        slot = lax.rem(b, SENDS)
        return pltpu.make_async_remote_copy(
            src_ref=bsend.at[slot], dst_ref=grads.at[b], send_sem=send_b.at[slot], recv_sem=recv_b.at[b],
            device_id={"pp": me - 1}, device_id_type=MESH,
        )

    def put_slopes(b):
        slot = lax.rem(b, OUT)
        return pltpu.make_async_copy(slopes.at[IN + slot], slopes_hbm.at[b], put_s.at[slot])

    def put_acts(b):
        slot = lax.rem(b, OUT)
        return pltpu.make_async_copy(acts.at[slot], acts_hbm.at[b], put_a.at[slot])

    def put_dgus(b):
        slot = lax.rem(b, 2)
        return pltpu.make_async_copy(dgus.at[slot], dgus_hbm.at[b], put_d.at[slot])

    def get_slopes(b):
        slot = lax.rem(b, IN)
        return pltpu.make_async_copy(slopes_hbm.at[b], slopes.at[slot], get_s.at[slot])

    def get_terms(k):
        side = lax.rem(k, 2)
        copies = []
        for j in range(blocks):
            b = k * blocks + j
            copies.append(pltpu.make_async_copy(acts_hbm.at[b], acts_in.at[side, j], get_a.at[side, j]))
            copies.append(pltpu.make_async_copy(dgus_hbm.at[b], dgus_in.at[side, j], get_d.at[side, j]))
        return copies

    @pl.when(first)
    def _():
        x_copy(0).start()

    for c in range(pieces):
        at = pl.ds(c * LANES, LANES)
        pltpu.make_async_copy(wg_ref.at[0, :, at], wgu.at[:, pl.ds(2 * c * LANES, LANES)], w_sem).start()
        pltpu.make_async_copy(wu_ref.at[0, :, at], wgu.at[:, pl.ds((2 * c + 1) * LANES, LANES)], w_sem).start()
    pltpu.make_async_copy(wd_ref.at[0], wd, wd_sem).start()

    barrier = pltpu.get_barrier_semaphore()

    @pl.when(me > 0)
    def _():
        pl.semaphore_signal(barrier, inc=1, device_id={"pp": me - 1}, device_id_type=MESH)

    @pl.when(me < stages - 1)
    def _():
        pl.semaphore_signal(barrier, inc=1, device_id={"pp": me + 1}, device_id_type=MESH)

    @pl.when(first)
    def _():
        @pl.loop(1, total_blocks)
        def _(b):
            x_copy(b).start()

    @pl.when(last)
    def _():
        @pl.loop(0, total_blocks)
        def _(b):
            dy_copy(b).start()

    pltpu.make_async_copy(wgu, wgu, w_sem).wait()
    pltpu.make_async_copy(wd_ref.at[0], wd, wd_sem).wait()

    def turn_weights():
        acc_gu[...] = jnp.zeros_like(acc_gu)
        acc_d[...] = jnp.zeros_like(acc_d)
        for c in range(pieces):
            at = pl.ds(c * LANES, LANES)
            wd_t[:, at] = wd[at, :].T
        for c in range(2 * pieces):
            at = pl.ds(c * LANES, LANES)
            wgu_t[at, :] = wgu[:, at].T

    @pl.when(me > 0)
    def _():
        turn_weights()

    pl.semaphore_wait(barrier, jnp.where(first | last, 1, 2))

    def gated(gu, n):
        g = jnp.concatenate([gu[:, 2 * i * LANES:(2 * i + 1) * LANES] for i in range(n)], axis=1)
        u = jnp.concatenate([gu[:, (2 * i + 1) * LANES:(2 * i + 2) * LANES] for i in range(n)], axis=1)
        return g, u, 0.5 * jnp.tanh(0.5 * g) + 0.5

    def f_arrive(b):
        @pl.when(first)
        def _():
            x_copy(b).wait()

        @pl.when(me > 0)
        def _():
            f_copy(b).wait_recv()

        @pl.when(b >= OUT)
        def _():
            put_acts(b - OUT).wait()

        @pl.when((me < stages - 1) & (b >= OUT))
        def _():
            put_slopes(b - OUT).wait()

        @pl.when((me < stages - 1) & (b >= SENDS))
        def _():
            f_copy(b - SENDS).wait_send()

    def f_norm(b):
        h = hs[b].astype(F32)
        scale = lax.rsqrt(jnp.mean(h * h, -1, keepdims=True) + EPS)
        acts[lax.rem(b, OUT), :, ff:] = (h * scale).astype(BF16)

    def f_chunk(b, c, w, to):
        slot = lax.rem(b, OUT)
        gu = dot(acts[slot, :, ff:], wgu[:, 2 * c:2 * c + 2 * w])
        g, u, s = gated(gu, w // LANES)
        silu = g * s
        slopes[to, :, c:c + w] = silu
        slopes[to, :, ff + c:ff + c + w] = u * (s + silu * (1.0 - s))
        acts[slot, :, c:c + w] = (silu * u).astype(BF16)

    def f_out(b):
        y = dot(acts[lax.rem(b, OUT), :, :ff], wd[...]).astype(BF16)
        fsend[lax.rem(b, SENDS)] = (hs[b].astype(F32) + y.astype(F32)).astype(BF16)

    def forward(b):
        f_arrive(b)
        f_norm(b)
        to = jnp.where(last, lax.rem(b, IN), IN + lax.rem(b, OUT))
        for c, w in wide:
            f_chunk(b, c, w, to)
        f_out(b)

        @pl.when(me < stages - 1)
        def _():
            f_copy(b).start()
            put_slopes(b).start()

        put_acts(b).start()

    def b_arrive(b):
        @pl.when(last)
        def _():
            dy_copy(b).wait()

        @pl.when(me < stages - 1)
        def _():
            @pl.when(b + IN - 1 < total_blocks)
            def _():
                get_slopes(b + IN - 1).start()

            pltpu.make_async_remote_copy(
                src_ref=bsend.at[0], dst_ref=grads.at[b], send_sem=send_b.at[0], recv_sem=recv_b.at[b],
                device_id={"pp": me + 1}, device_id_type=MESH,
            ).wait_recv()
            get_slopes(b).wait()

        @pl.when(b >= 2)
        def _():
            put_dgus(b - 2).wait()

        @pl.when((me > 0) & (b >= SENDS))
        def _():
            b_copy(b - SENDS).wait_send()

    def b_chunk(b, c, w):
        slot, come = lax.rem(b, 2), lax.rem(b, IN)
        dact = dot(grads[b], wd_t[:, c:c + w]).astype(BF16).astype(F32)
        dgate = (dact * slopes[come, :, ff + c:ff + c + w]).astype(BF16)
        dup = (dact * slopes[come, :, c:c + w]).astype(BF16)
        for i in range(w // LANES):
            at = 2 * c + 2 * i * LANES
            dgus[slot, :, at:at + LANES] = dgate[:, i * LANES:(i + 1) * LANES]
            dgus[slot, :, at + LANES:at + 2 * LANES] = dup[:, i * LANES:(i + 1) * LANES]

    def b_out(b):
        da = dot(dgus[lax.rem(b, 2)], wgu_t[...]).astype(BF16).astype(F32)
        h = hs[b].astype(F32)
        scale = lax.rsqrt(jnp.mean(h * h, -1, keepdims=True) + EPS)
        pull = jnp.mean(da * h, -1, keepdims=True) * (scale * scale * scale)
        dh = (da * scale - h * pull).astype(BF16).astype(F32)
        bsend[lax.rem(b, SENDS)] = (grads[b].astype(F32) + dh).astype(BF16)

    def backward(b):
        b_arrive(b)
        for c, w in wide:
            b_chunk(b, c, w)
        b_out(b)

        @pl.when(me > 0)
        def _():
            b_copy(b).start()

        put_dgus(b).start()

    tokens = rows * blocks

    def weight(k):
        side = lax.rem(k, 2)

        @pl.when(k + 1 < micro)
        def _():
            for copy in get_terms(k + 1):
                copy.start()

        turned[1] = grads[pl.ds(k * blocks, blocks)].reshape(tokens, d).T
        for copy in get_terms(k):
            copy.wait()
        turned[0] = acts_in[side, :, :, ff:].reshape(tokens, d).T
        for c in range(0, 2 * ff, 2 * LANES):
            term = dot(turned[0], dgus_in[side, :, :, c:c + 2 * LANES].reshape(tokens, -1))
            acc_gu[:, c:c + 2 * LANES] += term.astype(BF16).astype(F32)
        for c, w in wide:
            term = dot(turned[1], acts_in[side, :, :, c:c + w].reshape(tokens, -1))
            acc_d[:, c:c + w] += term.astype(BF16).astype(F32)

    def mine(table):
        return sum(jnp.where(me == i, entry, 0) for i, entry in enumerate(table))

    ahead, lag = mine(AHEAD), mine(LAG)

    @pl.loop(0, total_blocks + max(a + b for a, b in zip(AHEAD, LAG)))
    def _(t):
        b = t - ahead
        late = b - lag

        @pl.when(first & (t == 2))
        def _():
            turn_weights()

        @pl.when((me < stages - 1) & (b == -1))
        def _():
            for i in range(IN - 1):
                get_slopes(i).start()

        @pl.when(t == total_blocks)
        def _():
            for i in range(OUT):
                put_acts(total_blocks - OUT + i).wait()

        @pl.when((me < stages - 1) & (t == total_blocks))
        def _():
            for i in range(OUT):
                put_slopes(total_blocks - OUT + i).wait()

        to_f, to_b = t < total_blocks, (b >= 0) & (b < total_blocks)

        @pl.when(to_b)
        def _():
            backward(b)

        @pl.when(b == total_blocks)
        def _():
            put_dgus(total_blocks - 2).wait()
            put_dgus(total_blocks - 1).wait()

        @pl.when(to_f)
        def _():
            forward(t)

        @pl.when(late == 0)
        def _():
            for copy in get_terms(0):
                copy.start()

        @pl.when((late >= 0) & (late < total_blocks) & (lax.rem(late, blocks) == blocks - 1))
        def _():
            weight(late // blocks)

    copies = []
    spare = micro % 2

    def out(src, dst):
        copies.append(pltpu.make_async_copy(src, dst, out_sem.at[len(copies)]))
        copies[-1].start()

    for j in range(blocks):
        at = slice(j * rows, (j + 1) * rows)
        for c in range(pieces):
            dgus_in[spare, j, :, c * LANES:(c + 1) * LANES] = acc_gu[at, 2 * c * LANES:(2 * c + 1) * LANES].astype(BF16)
            dgus_in[spare, j, :, ff + c * LANES:ff + (c + 1) * LANES] = acc_gu[at, (2 * c + 1) * LANES:(2 * c + 2) * LANES].astype(BF16)
        out(dgus_in.at[spare, j, :, pl.ds(0, ff)], out_g.at[0, pl.ds(j * rows, rows)])
        out(dgus_in.at[spare, j, :, pl.ds(ff, ff)], out_u.at[0, pl.ds(j * rows, rows)])
    for c in range(pieces):
        at = slice(c * LANES, (c + 1) * LANES)
        wd[at, :] = acc_d[:, at].astype(BF16).T
    out(wd, out_d.at[0])

    @pl.when(me < stages - 1)
    def _():
        @pl.loop(total_blocks - SENDS, total_blocks)
        def _(b):
            f_copy(b).wait_send()

    @pl.when(me > 0)
    def _():
        @pl.loop(total_blocks - SENDS, total_blocks)
        def _(b):
            b_copy(b).wait_send()

    for copy in copies:
        copy.wait()


def solution(mesh):
    stages = mesh.shape["pp"]

    def step(x, dy, w_gate, w_up, w_down):
        micro, tokens, d = x.shape
        ff = w_gate.shape[-1]
        rows = tokens // BLOCKS
        count = micro * BLOCKS
        any_space = pl.BlockSpec(memory_space=pl.ANY)
        out_g, out_u, out_d, *_ = pl.pallas_call(
            functools.partial(kernel, stages, micro, BLOCKS),
            out_shape=(
                jax.ShapeDtypeStruct((1, d, ff), BF16),
                jax.ShapeDtypeStruct((1, d, ff), BF16),
                jax.ShapeDtypeStruct((1, ff, d), BF16),
                jax.ShapeDtypeStruct((count, rows, 2 * ff), F32),
                jax.ShapeDtypeStruct((count, rows, ff + d), BF16),
                jax.ShapeDtypeStruct((count, rows, 2 * ff), BF16),
            ),
            in_specs=[any_space] * 5,
            out_specs=(any_space,) * 6,
            scratch_shapes=[
                pltpu.VMEM((d, 2 * ff), BF16),
                pltpu.VMEM((ff, d), BF16),
                pltpu.VMEM((2 * ff, d), BF16),
                pltpu.VMEM((d, ff), BF16),
                pltpu.VMEM((count, rows, d), BF16),
                pltpu.VMEM((count, rows, d), BF16),
                pltpu.VMEM((SENDS, rows, d), BF16),
                pltpu.VMEM((SENDS, rows, d), BF16),
                pltpu.VMEM((IN + OUT, rows, 2 * ff), F32),
                pltpu.VMEM((OUT, rows, ff + d), BF16),
                pltpu.VMEM((2, rows, 2 * ff), BF16),
                pltpu.VMEM((2, BLOCKS, rows, ff + d), BF16),
                pltpu.VMEM((2, BLOCKS, rows, 2 * ff), BF16),
                pltpu.VMEM((2, d, tokens), BF16),
                pltpu.VMEM((d, 2 * ff), F32),
                pltpu.VMEM((d, ff), F32),
                pltpu.SemaphoreType.DMA,
                pltpu.SemaphoreType.DMA,
                pltpu.SemaphoreType.DMA((2 * BLOCKS + 1,)),
                pltpu.SemaphoreType.DMA((count,)),
                pltpu.SemaphoreType.DMA((count,)),
                pltpu.SemaphoreType.DMA((SENDS,)),
                pltpu.SemaphoreType.DMA((SENDS,)),
                pltpu.SemaphoreType.DMA((OUT,)),
                pltpu.SemaphoreType.DMA((OUT,)),
                pltpu.SemaphoreType.DMA((2,)),
                pltpu.SemaphoreType.DMA((IN,)),
                pltpu.SemaphoreType.DMA((2, BLOCKS)),
                pltpu.SemaphoreType.DMA((2, BLOCKS)),
            ],
            compiler_params=pltpu.CompilerParams(collective_id=0, has_side_effects=True, vmem_limit_bytes=67_043_328),
            name="stage",
        )(x.reshape(count, rows, d), dy.reshape(count, rows, d), w_gate, w_up, w_down)
        return out_g, out_u, out_d

    return jax.shard_map(
        step,
        mesh=mesh,
        in_specs=(P("rep", None, None),) * 2 + (P("pp", None, None),) * 3,
        out_specs=(P(("rep", "pp"), None, None),) * 3,
        check_vma=False,
    )
```

```python
import functools

import jax
import jax.numpy as jnp
from jax import lax
from jax.experimental import pallas as pl
from jax.experimental.pallas import tpu as pltpu
from jax.sharding import PartitionSpec as P

MESH = pl.DeviceIdType.MESH
F32, BF16 = jnp.float32, jnp.bfloat16
BLOCKS = 2
LANES = 128
AHEAD = (30, 26, 19, 17, 12, 10, 5, 1)
LAG = (4, 4, 12, 14, 19, 21, 32, 31)
SENDS = 4
IN, OUT = 3, 2
EPS = 1e-6


def dot(a, b):
    return jnp.dot(a, b, preferred_element_type=F32)


def kernel(
    stages, micro, blocks,
    x_ref, dy_ref, wg_ref, wu_ref, wd_ref, out_g, out_u, out_d, slopes_hbm, acts_hbm, dgus_hbm,
    wgu, wd, wgu_t, wd_t, hs, grads, fsend, bsend, slopes, acts, dgus, acts_in, dgus_in, normed, acc_gu, acc_d,
    w_sem, wd_sem, out_sem, recv_f, recv_b, send_f, send_b, put_s, put_a, put_d, get_s, get_a, get_d,
):
    me = lax.axis_index("pp")
    rows, d = hs.shape[1:]
    ff = wd.shape[0]
    first, last = me == 0, me == stages - 1
    pieces = ff // LANES
    wide = [(c, min(2 * LANES, ff - c)) for c in range(0, ff, 2 * LANES)]
    total_blocks = micro * blocks

    def x_copy(b):
        return pltpu.make_async_copy(x_ref.at[b], hs.at[b], recv_f.at[b])

    def dy_copy(b):
        return pltpu.make_async_copy(dy_ref.at[b], grads.at[b], recv_b.at[b])

    def f_copy(b):
        slot = lax.rem(b, SENDS)
        return pltpu.make_async_remote_copy(
            src_ref=fsend.at[slot], dst_ref=hs.at[b], send_sem=send_f.at[slot], recv_sem=recv_f.at[b],
            device_id={"pp": me + 1}, device_id_type=MESH,
        )

    def b_copy(b):
        slot = lax.rem(b, SENDS)
        return pltpu.make_async_remote_copy(
            src_ref=bsend.at[slot], dst_ref=grads.at[b], send_sem=send_b.at[slot], recv_sem=recv_b.at[b],
            device_id={"pp": me - 1}, device_id_type=MESH,
        )

    def put_slopes(b):
        slot = lax.rem(b, OUT)
        return pltpu.make_async_copy(slopes.at[IN + slot], slopes_hbm.at[b], put_s.at[slot])

    def put_acts(b):
        slot = lax.rem(b, OUT)
        return pltpu.make_async_copy(acts.at[slot], acts_hbm.at[b], put_a.at[slot])

    def put_dgus(b):
        slot = lax.rem(b, 2)
        return pltpu.make_async_copy(dgus.at[slot], dgus_hbm.at[b], put_d.at[slot])

    def get_slopes(b):
        slot = lax.rem(b, IN)
        return pltpu.make_async_copy(slopes_hbm.at[b], slopes.at[slot], get_s.at[slot])

    def get_terms(k):
        side = lax.rem(k, 2)
        copies = []
        for j in range(blocks):
            b = k * blocks + j
            copies.append(pltpu.make_async_copy(acts_hbm.at[b], acts_in.at[side, j], get_a.at[side, j]))
            copies.append(pltpu.make_async_copy(dgus_hbm.at[b], dgus_in.at[side, j], get_d.at[side, j]))
        return copies

    @pl.when(first)
    def _():
        x_copy(0).start()

    for c in range(pieces):
        at = pl.ds(c * LANES, LANES)
        pltpu.make_async_copy(wg_ref.at[0, :, at], wgu.at[:, pl.ds(2 * c * LANES, LANES)], w_sem).start()
        pltpu.make_async_copy(wu_ref.at[0, :, at], wgu.at[:, pl.ds((2 * c + 1) * LANES, LANES)], w_sem).start()
    pltpu.make_async_copy(wd_ref.at[0], wd, wd_sem).start()

    barrier = pltpu.get_barrier_semaphore()

    @pl.when(me > 0)
    def _():
        pl.semaphore_signal(barrier, inc=1, device_id={"pp": me - 1}, device_id_type=MESH)

    @pl.when(me < stages - 1)
    def _():
        pl.semaphore_signal(barrier, inc=1, device_id={"pp": me + 1}, device_id_type=MESH)

    @pl.when(first)
    def _():
        @pl.loop(1, total_blocks)
        def _(b):
            x_copy(b).start()

    @pl.when(last)
    def _():
        @pl.loop(0, total_blocks)
        def _(b):
            dy_copy(b).start()

    pltpu.make_async_copy(wgu, wgu, w_sem).wait()
    pltpu.make_async_copy(wd_ref.at[0], wd, wd_sem).wait()

    def turn_weights():
        acc_gu[...] = jnp.zeros_like(acc_gu)
        acc_d[...] = jnp.zeros_like(acc_d)
        for c in range(pieces):
            at = pl.ds(c * LANES, LANES)
            wd_t[:, at] = wd[at, :].T
        for c in range(2 * pieces):
            at = pl.ds(c * LANES, LANES)
            wgu_t[at, :] = wgu[:, at].T

    @pl.when(me > 0)
    def _():
        turn_weights()

    pl.semaphore_wait(barrier, jnp.where(first | last, 1, 2))

    def gated(gu, n):
        g = jnp.concatenate([gu[:, 2 * i * LANES:(2 * i + 1) * LANES] for i in range(n)], axis=1)
        u = jnp.concatenate([gu[:, (2 * i + 1) * LANES:(2 * i + 2) * LANES] for i in range(n)], axis=1)
        return g, u, 0.5 * jnp.tanh(0.5 * g) + 0.5

    def f_arrive(b):
        @pl.when(first)
        def _():
            x_copy(b).wait()

        @pl.when(me > 0)
        def _():
            f_copy(b).wait_recv()

        @pl.when(b >= OUT)
        def _():
            put_acts(b - OUT).wait()

        @pl.when((me < stages - 1) & (b >= OUT))
        def _():
            put_slopes(b - OUT).wait()

        @pl.when((me < stages - 1) & (b >= SENDS))
        def _():
            f_copy(b - SENDS).wait_send()

    def turned(block):
        return jnp.concatenate([block[:, c:c + rows].T for c in range(0, d, rows)], axis=1)

    def upright(parts):
        return jnp.concatenate(
            [jnp.concatenate([part[:, c:c + rows] for part in parts], axis=1) for c in range(0, d, rows)], axis=0
        )

    def f_norm(b):
        h = hs[b].astype(F32)
        scale = lax.rsqrt(jnp.mean(h * h, -1, keepdims=True) + EPS)
        a = (h * scale).astype(BF16)
        normed[...] = a
        acts[lax.rem(b, OUT), :, ff:] = turned(a)

    def f_chunk(b, c, w, to):
        slot = lax.rem(b, OUT)
        gu = dot(normed[...], wgu[:, 2 * c:2 * c + 2 * w])
        g, u, s = gated(gu, w // LANES)
        silu = g * s
        slopes[to, :, c:c + w] = silu
        slopes[to, :, ff + c:ff + c + w] = u * (s + silu * (1.0 - s))
        acts[slot, :, c:c + w] = (silu * u).astype(BF16)

    def f_out(b):
        y = dot(acts[lax.rem(b, OUT), :, :ff], wd[...]).astype(BF16)
        fsend[lax.rem(b, SENDS)] = (hs[b].astype(F32) + y.astype(F32)).astype(BF16)

    def forward(b):
        f_arrive(b)
        f_norm(b)
        to = jnp.where(last, lax.rem(b, IN), IN + lax.rem(b, OUT))
        for c, w in wide:
            f_chunk(b, c, w, to)
        f_out(b)

        @pl.when(me < stages - 1)
        def _():
            f_copy(b).start()
            put_slopes(b).start()

        put_acts(b).start()

    def b_arrive(b):
        @pl.when(last)
        def _():
            dy_copy(b).wait()

        @pl.when(me < stages - 1)
        def _():
            @pl.when(b + IN - 1 < total_blocks)
            def _():
                get_slopes(b + IN - 1).start()

            pltpu.make_async_remote_copy(
                src_ref=bsend.at[0], dst_ref=grads.at[b], send_sem=send_b.at[0], recv_sem=recv_b.at[b],
                device_id={"pp": me + 1}, device_id_type=MESH,
            ).wait_recv()
            get_slopes(b).wait()

        @pl.when(b >= 2)
        def _():
            put_dgus(b - 2).wait()

        @pl.when((me > 0) & (b >= SENDS))
        def _():
            b_copy(b - SENDS).wait_send()

    def b_chunk(b, c, w):
        slot, come = lax.rem(b, 2), lax.rem(b, IN)
        dact = dot(grads[b], wd_t[:, c:c + w]).astype(BF16).astype(F32)
        dgate = (dact * slopes[come, :, ff + c:ff + c + w]).astype(BF16)
        dup = (dact * slopes[come, :, c:c + w]).astype(BF16)
        for i in range(w // LANES):
            at = 2 * c + 2 * i * LANES
            dgus[slot, :, at:at + LANES] = dgate[:, i * LANES:(i + 1) * LANES]
            dgus[slot, :, at + LANES:at + 2 * LANES] = dup[:, i * LANES:(i + 1) * LANES]

    def b_out(b):
        da = dot(dgus[lax.rem(b, 2)], wgu_t[...]).astype(BF16).astype(F32)
        h = hs[b].astype(F32)
        scale = lax.rsqrt(jnp.mean(h * h, -1, keepdims=True) + EPS)
        pull = jnp.mean(da * h, -1, keepdims=True) * (scale * scale * scale)
        dh = (da * scale - h * pull).astype(BF16).astype(F32)
        bsend[lax.rem(b, SENDS)] = (grads[b].astype(F32) + dh).astype(BF16)
        hs[b] = turned(grads[b])

    def backward(b):
        b_arrive(b)
        for c, w in wide:
            b_chunk(b, c, w)
        b_out(b)

        @pl.when(me > 0)
        def _():
            b_copy(b).start()

        put_dgus(b).start()

    tokens = rows * blocks

    def weight(k):
        side = lax.rem(k, 2)

        @pl.when(k + 1 < micro)
        def _():
            for copy in get_terms(k + 1):
                copy.start()

        for copy in get_terms(k):
            copy.wait()
        a_t = upright([acts_in[side, j, :, ff:] for j in range(blocks)])
        dy_t = upright([hs[k * blocks + j] for j in range(blocks)])
        for c in range(0, 2 * ff, 2 * LANES):
            term = dot(a_t, dgus_in[side, :, :, c:c + 2 * LANES].reshape(tokens, -1))
            acc_gu[:, c:c + 2 * LANES] += term.astype(BF16).astype(F32)
        for c, w in wide:
            term = dot(dy_t, acts_in[side, :, :, c:c + w].reshape(tokens, -1))
            acc_d[:, c:c + w] += term.astype(BF16).astype(F32)

    def mine(table):
        return sum(jnp.where(me == i, entry, 0) for i, entry in enumerate(table))

    ahead, lag = mine(AHEAD), mine(LAG)

    @pl.loop(0, total_blocks + max(a + b for a, b in zip(AHEAD, LAG)))
    def _(t):
        b = t - ahead
        late = b - lag

        @pl.when(first & (t == 2))
        def _():
            turn_weights()

        @pl.when((me < stages - 1) & (b == -1))
        def _():
            for i in range(IN - 1):
                get_slopes(i).start()

        @pl.when(t == total_blocks)
        def _():
            for i in range(OUT):
                put_acts(total_blocks - OUT + i).wait()

        @pl.when((me < stages - 1) & (t == total_blocks))
        def _():
            for i in range(OUT):
                put_slopes(total_blocks - OUT + i).wait()

        to_f, to_b = t < total_blocks, (b >= 0) & (b < total_blocks)

        @pl.when(to_b)
        def _():
            backward(b)

        @pl.when(b == total_blocks)
        def _():
            put_dgus(total_blocks - 2).wait()
            put_dgus(total_blocks - 1).wait()

        @pl.when(to_f)
        def _():
            forward(t)

        @pl.when(late == 0)
        def _():
            for copy in get_terms(0):
                copy.start()

        @pl.when((late >= 0) & (late < total_blocks) & (lax.rem(late, blocks) == blocks - 1))
        def _():
            weight(late // blocks)

    copies = []
    spare = micro % 2

    def out(src, dst):
        copies.append(pltpu.make_async_copy(src, dst, out_sem.at[len(copies)]))
        copies[-1].start()

    for j in range(blocks):
        at = slice(j * rows, (j + 1) * rows)
        for c in range(pieces):
            dgus_in[spare, j, :, c * LANES:(c + 1) * LANES] = acc_gu[at, 2 * c * LANES:(2 * c + 1) * LANES].astype(BF16)
            dgus_in[spare, j, :, ff + c * LANES:ff + (c + 1) * LANES] = acc_gu[at, (2 * c + 1) * LANES:(2 * c + 2) * LANES].astype(BF16)
        out(dgus_in.at[spare, j, :, pl.ds(0, ff)], out_g.at[0, pl.ds(j * rows, rows)])
        out(dgus_in.at[spare, j, :, pl.ds(ff, ff)], out_u.at[0, pl.ds(j * rows, rows)])
    for c in range(pieces):
        at = slice(c * LANES, (c + 1) * LANES)
        wd[at, :] = acc_d[:, at].astype(BF16).T
    out(wd, out_d.at[0])

    @pl.when(me < stages - 1)
    def _():
        @pl.loop(total_blocks - SENDS, total_blocks)
        def _(b):
            f_copy(b).wait_send()

    @pl.when(me > 0)
    def _():
        @pl.loop(total_blocks - SENDS, total_blocks)
        def _(b):
            b_copy(b).wait_send()

    for copy in copies:
        copy.wait()


def place(g_ref, u_ref, d_ref, out_g, out_u, out_d, buf_g, buf_u, buf_d, sem_in, sem_out):
    moves = []
    for ref, buf, out in ((g_ref, buf_g, out_g), (u_ref, buf_u, out_u), (d_ref, buf_d, out_d)):
        rows = ref.shape[1] // 4
        for i in range(4):
            at, n = pl.ds(i * rows, rows), len(moves)
            moves.append((
                pltpu.make_async_copy(ref.at[0, at], buf.at[at], sem_in.at[n]),
                pltpu.make_async_copy(buf.at[at], out.at[0, at], sem_out.at[n]),
            ))
    for come, _ in moves:
        come.start()
    for come, go in moves:
        come.wait()
        go.start()
    for _, go in moves:
        go.wait()


def solution(mesh):
    stages = mesh.shape["pp"]

    def step(x, dy, w_gate, w_up, w_down):
        micro, tokens, d = x.shape
        ff = w_gate.shape[-1]
        rows = tokens // BLOCKS
        count = micro * BLOCKS
        any_space = pl.BlockSpec(memory_space=pl.ANY)
        out_g, out_u, out_d, *_ = pl.pallas_call(
            functools.partial(kernel, stages, micro, BLOCKS),
            out_shape=(
                jax.ShapeDtypeStruct((1, d, ff), BF16),
                jax.ShapeDtypeStruct((1, d, ff), BF16),
                jax.ShapeDtypeStruct((1, ff, d), BF16),
                jax.ShapeDtypeStruct((count, rows, 2 * ff), F32),
                jax.ShapeDtypeStruct((count, rows, ff + d), BF16),
                jax.ShapeDtypeStruct((count, rows, 2 * ff), BF16),
            ),
            in_specs=[any_space] * 5,
            out_specs=(any_space,) * 6,
            scratch_shapes=[
                pltpu.VMEM((d, 2 * ff), BF16),
                pltpu.VMEM((ff, d), BF16),
                pltpu.VMEM((2 * ff, d), BF16),
                pltpu.VMEM((d, ff), BF16),
                pltpu.VMEM((count, rows, d), BF16),
                pltpu.VMEM((count, rows, d), BF16),
                pltpu.VMEM((SENDS, rows, d), BF16),
                pltpu.VMEM((SENDS, rows, d), BF16),
                pltpu.VMEM((IN + OUT, rows, 2 * ff), F32),
                pltpu.VMEM((OUT, rows, ff + d), BF16),
                pltpu.VMEM((2, rows, 2 * ff), BF16),
                pltpu.VMEM((2, BLOCKS, rows, ff + d), BF16),
                pltpu.VMEM((2, BLOCKS, rows, 2 * ff), BF16),
                pltpu.VMEM((rows, d), BF16),
                pltpu.VMEM((d, 2 * ff), F32),
                pltpu.VMEM((d, ff), F32),
                pltpu.SemaphoreType.DMA,
                pltpu.SemaphoreType.DMA,
                pltpu.SemaphoreType.DMA((2 * BLOCKS + 1,)),
                pltpu.SemaphoreType.DMA((count,)),
                pltpu.SemaphoreType.DMA((count,)),
                pltpu.SemaphoreType.DMA((SENDS,)),
                pltpu.SemaphoreType.DMA((SENDS,)),
                pltpu.SemaphoreType.DMA((OUT,)),
                pltpu.SemaphoreType.DMA((OUT,)),
                pltpu.SemaphoreType.DMA((2,)),
                pltpu.SemaphoreType.DMA((IN,)),
                pltpu.SemaphoreType.DMA((2, BLOCKS)),
                pltpu.SemaphoreType.DMA((2, BLOCKS)),
            ],
            compiler_params=pltpu.CompilerParams(collective_id=0, has_side_effects=True, vmem_limit_bytes=67_043_328),
            name="stage",
        )(x.reshape(count, rows, d), dy.reshape(count, rows, d), w_gate, w_up, w_down)
        results = (out_g, out_u, out_d)
        return pl.pallas_call(
            place,
            out_shape=tuple(jax.ShapeDtypeStruct(r.shape, r.dtype) for r in results),
            in_specs=[any_space] * 3,
            out_specs=(any_space,) * 3,
            scratch_shapes=[
                *(pltpu.VMEM(r.shape[1:], r.dtype) for r in results),
                pltpu.SemaphoreType.DMA((12,)),
                pltpu.SemaphoreType.DMA((12,)),
            ],
            name="place",
        )(*results)

    return jax.shard_map(
        step,
        mesh=mesh,
        in_specs=(P("rep", None, None),) * 2 + (P("pp", None, None),) * 3,
        out_specs=(P(("rep", "pp"), None, None),) * 3,
        check_vma=False,
    )
```
